256 devices in a mesh: gx: 8 (over z), gy: 8 (over y, x_hi), gz: 4 (over x_lo, core).
Axes of the slice: x: 4 (x_hi: 2, x_lo: 2; x = x_hi * 2 + x_lo), y: 4, z: 8, core: 2. Of those that a mesh axis runs over, the one named last changes fastest.
Arguments:
- hidden_acts: bfloat16 [4, 8, 8, 256, 16384], P('gz', 'gy', 'gx'), may hold values from -6 to 6
- output_grad: bfloat16 [4, 8, 8, 256, 32], P('gz', 'gy', 'gx'), may hold values from -6 to 6
- weights: bfloat16 [4, 8, 8, 32, 16384], P('gz', 'gy', 'gx'), may hold values from -6 to 6
- momentum: bfloat16 [4, 8, 8, 32, 16384], P('gz', 'gy', 'gx'), may hold values from -48 to 48
- worker_of_slot: int32 [256], replicated, may hold values from 0 to 255, each once
- round_shift: int32 [8], replicated, may hold values from 0 to 7, as said below
Outputs:
- mixed: bfloat16 [8, 8, 4, 32, 16384], P('gx', 'gy', 'gz')
- new_momentum: bfloat16 [4, 8, 8, 32, 16384], P('gz', 'gy', 'gx')
The draws below stay inside these ranges and needn't reach their ends.
Inputs may be any that keep to these rules, and one draw needn't show every extreme that they name: `round_shift`: each entry is below log2 of 256, so offsets are powers of two below 256; some round has offset 256 / 2 and some round offset 1.
All inputs are finite; a program needn't handle non-finite values.
Results may differ from the reference program's by a relative error of at most 0.0081.
Values may be sent and summed in bfloat16 or wider, within the bound.
No kernel may reach another device: no remote copies, remote signals or barrier semaphores. Data moves between devices by JAX's collectives and lax.ppermute only.
A program may use at most 64 MiB of HBM per device.

```python
import jax
import jax.numpy as jnp
from jax import lax

FF = 16384
ROWS = 32
TOK = 256
ROUNDS = 8
WORKERS = 256
N_GX = 8
N_GY = 8
N_GZ = 4


def draw_round_shift(key, part):
    levels = WORKERS.bit_length() - 1
    first_key = jax.random.fold_in(key, 11)
    second_key = jax.random.fold_in(key, 23)
    values = jax.random.randint(first_key, (ROUNDS,), 0, levels, dtype=jnp.int32)
    order = jax.random.permutation(second_key, ROUNDS)
    values = values.at[order[0]].set(jnp.int32(levels - 1))
    values = values.at[order[1]].set(jnp.int32(0))
    return values.astype(jnp.int32)


def shard_levels(rng, shape, split, least, top_value):
    def one(position, shards_of):
        heights = jax.random.uniform(jax.random.fold_in(jax.random.fold_in(rng, 6), position), (shards_of,), jnp.float32, least / len(split), top_value / len(split))
        return jnp.repeat(jnp.exp(heights), shape[position] // shards_of).reshape((-1,) + (1,) * (len(shape) - position - 1))

    level = one(*split[0])
    for cut in split[1:]:
        level = level * one(*cut)
    return level


def scatter_about(key, extent, deviation, most, cuts=(), kind=jnp.bfloat16):
    entries = deviation * jax.random.normal(key, extent, jnp.float32)
    if cuts:
        entries = entries * shard_levels(key, extent, cuts, -0.22, 0.18)
    return jnp.clip(entries, -most, most).astype(kind)


def setup_inputs(seed: int = 0) -> dict:
    seeds = jax.random.split(jax.random.key(seed), 7)
    return {
        "hidden_acts": scatter_about(seeds[0], (N_GZ, N_GY, N_GX, TOK, FF), 1.0, 6.0, ((0, 4), (1, 8), (2, 8))),
        "output_grad": scatter_about(seeds[1], (N_GZ, N_GY, N_GX, TOK, ROWS), 1.0, 6.0, ((0, 4), (1, 8), (2, 8))),
        "weights": scatter_about(seeds[2], (N_GZ, N_GY, N_GX, ROWS, FF), 1.0, 6.0, ((0, 4), (1, 8), (2, 8))),
        "momentum": scatter_about(seeds[3], (N_GZ, N_GY, N_GX, ROWS, FF), 8.0, 48.0, ((0, 4), (1, 8), (2, 8))),
        "worker_of_slot": jax.random.permutation(seeds[4], WORKERS).astype(jnp.int32),
        "round_shift": draw_round_shift(jax.random.fold_in(seeds[6], 71), 0),
    }


learn_rate = 0.01
beta_keep = 0.9


def local_step(items):
    hidden, grad_out, weight, moment = items
    grad = lax.dot_general(grad_out, hidden, (((0,), (0,)), ((), ())), preferred_element_type=jnp.float32)
    velocity = beta_keep * moment.astype(jnp.float32) + grad
    stepped = (weight.astype(jnp.float32) - learn_rate * velocity).astype(jnp.bfloat16)
    return stepped, velocity.astype(jnp.bfloat16)


def reference(hidden_acts, output_grad, weights, momentum, worker_of_slot, round_shift):
    workers = N_GX * N_GY * N_GZ
    hidden = hidden_acts.reshape(workers, TOK, FF)
    grad_out = output_grad.reshape(workers, TOK, ROWS)
    weight = weights.reshape(workers, ROWS, FF)
    moment = momentum.reshape(workers, ROWS, FF)
    stepped, new_moment = lax.map(local_step, (hidden, grad_out, weight, moment))
    replica = jnp.zeros_like(stepped).at[worker_of_slot].set(stepped)
    for step in range(ROUNDS):
        offset = jnp.left_shift(jnp.int32(1), round_shift[step].astype(jnp.int32))
        peer = jnp.roll(replica, offset, axis=0)
        replica = ((replica.astype(jnp.float32) + peer.astype(jnp.float32)) * 0.5).astype(jnp.bfloat16)
    mixed = replica.reshape(N_GX, N_GY, N_GZ, ROWS, FF)
    return mixed, new_moment.reshape(N_GZ, N_GY, N_GX, ROWS, FF)
```

```python
import functools

import jax
import jax.numpy as jnp
from jax import lax
from jax.experimental import pallas as pl
from jax.experimental.pallas import tpu as pltpu
from jax.sharding import PartitionSpec as P

CHUNKS = 1
BLOCK = 2048
LANES = 128
SUB = 8

learn_rate = 0.01
beta_keep = 0.9


def step_kernel(grad_out_ref, hidden_ref, weight_ref, moment_ref, *rest):
    new_moment_ref, pieces_ref = rest[-2:]
    grad = jnp.dot(grad_out_ref[...], hidden_ref[...], preferred_element_type=jnp.float32)
    velocity = beta_keep * moment_ref[...].astype(jnp.float32) + grad
    new_moment_ref[...] = velocity.astype(jnp.bfloat16)
    stepped = (weight_ref[...].astype(jnp.float32) - learn_rate * velocity).astype(jnp.bfloat16)
    groups, count, _, width = pieces_ref.shape
    for group in range(groups):
        for at in range(count):
            pieces_ref[group, at] = stepped[
                group * SUB : (group + 1) * SUB, at * width : (at + 1) * width
            ]


def local_step(chunk, grad_out, hidden, weight, moment, held):
    rows, cols = weight.shape
    tokens = hidden.shape[0]
    span = cols // CHUNKS
    steps = span // BLOCK
    groups = rows // SUB
    width = span * groups // 256
    first = chunk * steps
    block = pl.BlockSpec((rows, BLOCK), lambda i: (0, first + i))
    in_specs = [
        pl.BlockSpec((rows, tokens), lambda i: (0, 0)),
        pl.BlockSpec((tokens, BLOCK), lambda i: (0, first + i)),
        block,
        block,
    ]
    operands = [grad_out, hidden, weight, moment]
    aliases = {}
    if held is not None:
        in_specs.append(pl.BlockSpec(memory_space=pl.ANY))
        operands.append(held)
        aliases = {4: 0}
    return pl.pallas_call(
        step_kernel,
        grid=(steps,),
        in_specs=in_specs,
        out_specs=(
            block,
            pl.BlockSpec((groups, BLOCK // width, SUB, width), lambda i: (0, i, 0, 0)),
        ),
        out_shape=(
            jax.ShapeDtypeStruct((rows, cols), jnp.bfloat16),
            jax.ShapeDtypeStruct((groups, span // width, SUB, width), jnp.bfloat16),
        ),
        input_output_aliases=aliases,
        name=f"local_step_{chunk}",
    )(*operands)


def mixing_kernel(shift_ref, worker_ref, out_ref):
    workers = worker_ref.shape[1]
    half = workers // 2
    row = lax.broadcasted_iota(jnp.int32, (workers, workers), 0)
    col = lax.broadcasted_iota(jnp.int32, (workers, workers), 1)
    gap = (row - col) & (workers - 1)
    mix = (row == worker_ref[...]).astype(jnp.float32)
    for step in range(shift_ref.shape[0]):
        offset = jnp.left_shift(jnp.int32(1), shift_ref[step])
        one = ((gap == 0) | (gap == offset)).astype(jnp.bfloat16)
        mix = jnp.dot(one, mix.astype(jnp.bfloat16), preferred_element_type=jnp.float32)
    mix = mix[:half].astype(jnp.bfloat16)
    wide = workers * SUB
    spread_col = (
        lax.broadcasted_iota(jnp.int32, (workers, wide), 1) // SUB
        == lax.broadcasted_iota(jnp.int32, (workers, wide), 0)
    ).astype(jnp.bfloat16)
    wide_mix = jnp.dot(mix, spread_col, preferred_element_type=jnp.float32)
    wide_mix = wide_mix * (1.0 / workers)
    same = (
        lax.broadcasted_iota(jnp.int32, (SUB, wide), 1) & (SUB - 1)
        == lax.broadcasted_iota(jnp.int32, (SUB, wide), 0)
    )
    for at in range(half):
        line = jnp.broadcast_to(wide_mix[at : at + 1], (SUB, wide))
        out_ref[at * SUB : (at + 1) * SUB] = jnp.where(same, line, 0.0).astype(jnp.bfloat16)


def mixing(round_shift, held):
    workers = held.shape[1]
    return pl.pallas_call(
        mixing_kernel,
        in_specs=[
            pl.BlockSpec(memory_space=pltpu.SMEM),
            pl.BlockSpec(memory_space=pltpu.VMEM),
        ],
        out_specs=pl.BlockSpec(memory_space=pltpu.VMEM),
        out_shape=jax.ShapeDtypeStruct((workers * SUB // 2, workers * SUB), jnp.bfloat16),
        name="mixing",
    )(round_shift, held)


def mix_kernel(mix_ref, rows_ref, out_ref):
    mixed = jnp.dot(mix_ref[...], rows_ref[...], preferred_element_type=jnp.float32)
    mixed = mixed.astype(jnp.bfloat16)
    half = out_ref.shape[0] // 2
    out_ref[:half] = mixed
    out_ref[half:] = mixed


def mix(matrix, rows):
    return pl.pallas_call(
        mix_kernel,
        in_specs=[
            pl.BlockSpec(memory_space=pltpu.VMEM),
            pl.BlockSpec(memory_space=pltpu.VMEM),
        ],
        out_specs=pl.BlockSpec(memory_space=pltpu.VMEM),
        out_shape=jax.ShapeDtypeStruct(rows.shape, jnp.bfloat16),
        name="mix",
    )(matrix, rows)


def exchange(pieces):
    return lax.all_to_all(pieces, ("gx", "gy", "gz"), split_axis=0, concat_axis=0, tiled=True)


def shards(hidden_acts, output_grad, weights, momentum, worker_of_slot, round_shift):
    hidden = hidden_acts.reshape(hidden_acts.shape[-2:])
    grad_out = output_grad.reshape(output_grad.shape[-2:]).T
    weight = weights.reshape(weights.shape[-2:])
    moment = momentum.reshape(momentum.shape[-2:])
    count_x = lax.axis_size("gx")
    count_y = lax.axis_size("gy")
    count_z = lax.axis_size("gz")
    workers = count_x * count_y * count_z
    rows, cols = weight.shape
    groups = rows // SUB
    held = worker_of_slot.reshape(count_z, count_y, count_x).transpose(2, 1, 0)
    matrix = mixing(round_shift, held.reshape(1, workers))
    new_moment = None
    parts = []
    for chunk in range(CHUNKS):
        new_moment, pieces = local_step(chunk, grad_out, hidden, weight, moment, new_moment)
        parts.append(exchange(pieces.reshape(workers, SUB, -1)))
    mixed = []
    for part in parts:
        width = part.shape[-1]
        out = mix(matrix, part.reshape(workers * SUB, width))
        mixed.append(exchange(out.reshape(workers, SUB, width)))
    done = [
        part.reshape(groups, workers // groups, SUB, -1).transpose(0, 2, 1, 3).reshape(rows, -1)
        for part in mixed
    ]
    block = jnp.concatenate(done, axis=1) if CHUNKS > 1 else done[0]
    return (block.reshape(weights.shape), new_moment.reshape(momentum.shape))


def solution(mesh):
    placed = (
        P("gz", "gy", "gx", None, None),
        P("gz", "gy", "gx", None, None),
        P("gz", "gy", "gx", None, None),
        P("gz", "gy", "gx", None, None),
        P(),
        P(),
    )
    return jax.shard_map(
        shards,
        mesh=mesh,
        in_specs=placed,
        out_specs=(P("gx", "gy", "gz", None, None), P("gz", "gy", "gx", None, None)),
        check_vma=False,
    )
```

```python
import functools

import jax
import jax.numpy as jnp
from jax import lax
from jax.experimental import pallas as pl
from jax.experimental.pallas import tpu as pltpu
from jax.sharding import PartitionSpec as P

CHUNKS = 1
BLOCK = 2048
LANES = 128
SUB = 8

learn_rate = 0.01
beta_keep = 0.9


def step_kernel(grad_out_ref, hidden_ref, weight_ref, moment_ref, *rest):
    new_moment_ref, pieces_ref = rest[-2:]
    grad = jnp.dot(grad_out_ref[...], hidden_ref[...], preferred_element_type=jnp.float32)
    velocity = beta_keep * moment_ref[...].astype(jnp.float32) + grad
    new_moment_ref[...] = velocity.astype(jnp.bfloat16)
    stepped = (weight_ref[...].astype(jnp.float32) - learn_rate * velocity).astype(jnp.bfloat16)
    groups, count, _, width = pieces_ref.shape
    for group in range(groups):
        for at in range(count):
            pieces_ref[group, at] = stepped[
                group * SUB : (group + 1) * SUB, at * width : (at + 1) * width
            ]


def local_step(chunk, grad_out, hidden, weight, moment, held):
    rows, cols = weight.shape
    tokens = hidden.shape[0]
    span = cols // CHUNKS
    steps = span // BLOCK
    groups = rows // SUB
    width = span * groups // 256
    first = chunk * steps
    block = pl.BlockSpec((rows, BLOCK), lambda i: (0, first + i))
    in_specs = [
        pl.BlockSpec((rows, tokens), lambda i: (0, 0)),
        pl.BlockSpec((tokens, BLOCK), lambda i: (0, first + i)),
        block,
        block,
    ]
    operands = [grad_out, hidden, weight, moment]
    aliases = {}
    if held is not None:
        in_specs.append(pl.BlockSpec(memory_space=pl.ANY))
        operands.append(held)
        aliases = {4: 0}
    return pl.pallas_call(
        step_kernel,
        grid=(steps,),
        in_specs=in_specs,
        out_specs=(
            block,
            pl.BlockSpec((groups, BLOCK // width, SUB, width), lambda i: (0, i, 0, 0)),
        ),
        out_shape=(
            jax.ShapeDtypeStruct((rows, cols), jnp.bfloat16),
            jax.ShapeDtypeStruct((groups, span // width, SUB, width), jnp.bfloat16),
        ),
        input_output_aliases=aliases,
        compiler_params=pltpu.CompilerParams(vmem_limit_bytes=24 << 20),
        name=f"local_step_{chunk}",
    )(*[pltpu.with_memory_space_constraint(a, pltpu.HBM) for a in operands])


def mixing_kernel(shift_ref, worker_ref, out_ref):
    workers = worker_ref.shape[1]
    half = workers // 2
    row = lax.broadcasted_iota(jnp.int32, (workers, workers), 0)
    col = lax.broadcasted_iota(jnp.int32, (workers, workers), 1)
    gap = (row - col) & (workers - 1)
    mix = (row == worker_ref[...]).astype(jnp.float32)
    for step in range(shift_ref.shape[0]):
        offset = jnp.left_shift(jnp.int32(1), shift_ref[step])
        one = ((gap == 0) | (gap == offset)).astype(jnp.bfloat16)
        mix = jnp.dot(one, mix.astype(jnp.bfloat16), preferred_element_type=jnp.float32)
    mix = mix[:half].astype(jnp.bfloat16)
    wide = workers * SUB
    spread_col = (
        lax.broadcasted_iota(jnp.int32, (workers, wide), 1) // SUB
        == lax.broadcasted_iota(jnp.int32, (workers, wide), 0)
    ).astype(jnp.bfloat16)
    wide_mix = jnp.dot(mix, spread_col, preferred_element_type=jnp.float32)
    out_ref[...] = wide_mix * (1.0 / workers)


def mixing(round_shift, held):
    workers = held.shape[1]
    return pl.pallas_call(
        mixing_kernel,
        in_specs=[
            pl.BlockSpec(memory_space=pltpu.SMEM),
            pl.BlockSpec(memory_space=pltpu.VMEM),
        ],
        out_specs=pl.BlockSpec(memory_space=pltpu.VMEM),
        out_shape=pltpu.VMEM((workers // 2, workers * SUB), jnp.float32),
        compiler_params=pltpu.CompilerParams(vmem_limit_bytes=24 << 20),
        name="mixing",
    )(round_shift, held)


def mix_kernel(mix_ref, rows_ref, out_ref, full_ref):
    half, wide = mix_ref.shape
    same = (
        lax.broadcasted_iota(jnp.int32, (SUB, wide), 1) & (SUB - 1)
        == lax.broadcasted_iota(jnp.int32, (SUB, wide), 0)
    )
    for at in range(0, half, 2):
        lines = [
            jnp.where(same, jnp.broadcast_to(mix_ref[k : k + 1], (SUB, wide)), 0.0)
            for k in (at, at + 1)
        ]
        full_ref[at * SUB : (at + 2) * SUB] = jnp.concatenate(lines, axis=0).astype(jnp.bfloat16)
    mixed = jnp.dot(full_ref[...], rows_ref[...], preferred_element_type=jnp.float32)
    mixed = mixed.astype(jnp.bfloat16)
    out_ref[: half * SUB] = mixed
    out_ref[half * SUB :] = mixed


def mix(matrix, rows):
    half, wide = matrix.shape
    return pl.pallas_call(
        mix_kernel,
        in_specs=[
            pl.BlockSpec(memory_space=pltpu.VMEM),
            pl.BlockSpec(memory_space=pltpu.VMEM),
        ],
        out_specs=pl.BlockSpec(memory_space=pltpu.VMEM),
        out_shape=pltpu.VMEM(rows.shape, jnp.bfloat16),
        scratch_shapes=[pltpu.VMEM((half * SUB, wide), jnp.bfloat16)],
        compiler_params=pltpu.CompilerParams(vmem_limit_bytes=24 << 20),
        name="mix",
    )(
        pltpu.with_memory_space_constraint(matrix, pltpu.VMEM),
        pltpu.with_memory_space_constraint(rows, pltpu.VMEM),
    )


def exchange(pieces):
    return lax.all_to_all(pieces, ("gx", "gy", "gz"), split_axis=0, concat_axis=0, tiled=True)


def shards(hidden_acts, output_grad, weights, momentum, worker_of_slot, round_shift):
    hidden = hidden_acts.reshape(hidden_acts.shape[-2:])
    grad_out = output_grad.reshape(output_grad.shape[-2:]).T
    weight = weights.reshape(weights.shape[-2:])
    moment = momentum.reshape(momentum.shape[-2:])
    count_x = lax.axis_size("gx")
    count_y = lax.axis_size("gy")
    count_z = lax.axis_size("gz")
    workers = count_x * count_y * count_z
    rows, cols = weight.shape
    groups = rows // SUB
    held = worker_of_slot.reshape(count_z, count_y, count_x).transpose(2, 1, 0)
    matrix = mixing(round_shift, held.reshape(1, workers))
    new_moment = None
    parts = []
    for chunk in range(CHUNKS):
        new_moment, pieces = local_step(chunk, grad_out, hidden, weight, moment, new_moment)
        parts.append(exchange(pieces.reshape(workers, SUB, -1)))
    mixed = []
    for part in parts:
        width = part.shape[-1]
        out = mix(matrix, part.reshape(workers * SUB, width))
        mixed.append(exchange(out.reshape(workers, SUB, width)))
    done = [
        part.reshape(groups, workers // groups, SUB, -1).transpose(0, 2, 1, 3).reshape(rows, -1)
        for part in mixed
    ]
    block = jnp.concatenate(done, axis=1) if CHUNKS > 1 else done[0]
    return (block.reshape(weights.shape), new_moment.reshape(momentum.shape))


def solution(mesh):
    placed = (
        P("gz", "gy", "gx", None, None),
        P("gz", "gy", "gx", None, None),
        P("gz", "gy", "gx", None, None),
        P("gz", "gy", "gx", None, None),
        P(),
        P(),
    )
    return jax.shard_map(
        shards,
        mesh=mesh,
        in_specs=placed,
        out_specs=(P("gx", "gy", "gz", None, None), P("gz", "gy", "gx", None, None)),
        check_vma=False,
    )
```

```python
import functools

import jax
import jax.numpy as jnp
from jax import lax
from jax.experimental import pallas as pl
from jax.experimental.pallas import tpu as pltpu
from jax.sharding import PartitionSpec as P

CHUNKS = 1
BLOCK = 8192
LANES = 128
SUB = 8

learn_rate = 0.01
beta_keep = 0.9


def step_kernel(grad_out_ref, hidden_ref, weight_ref, moment_ref, *rest):
    new_moment_ref, pieces_ref = rest[-2:]
    grad = jnp.dot(grad_out_ref[...], hidden_ref[...], preferred_element_type=jnp.float32)
    velocity = beta_keep * moment_ref[...].astype(jnp.float32) + grad
    new_moment_ref[...] = velocity.astype(jnp.bfloat16)
    stepped = (weight_ref[...].astype(jnp.float32) - learn_rate * velocity).astype(jnp.bfloat16)
    groups, count, _, width = pieces_ref.shape
    for group in range(groups):
        for at in range(count):
            pieces_ref[group, at] = stepped[
                group * SUB : (group + 1) * SUB, at * width : (at + 1) * width
            ]


def local_step(chunk, grad_out, hidden, weight, moment, held):
    rows, cols = weight.shape
    tokens = hidden.shape[0]
    span = cols // CHUNKS
    steps = span // BLOCK
    groups = rows // SUB
    width = span * groups // 256
    first = chunk * steps
    block = pl.BlockSpec((rows, BLOCK), lambda i: (0, first + i))
    in_specs = [
        pl.BlockSpec((rows, tokens), lambda i: (0, 0)),
        pl.BlockSpec((tokens, BLOCK), lambda i: (0, first + i)),
        block,
        block,
    ]
    operands = [grad_out, hidden, weight, moment]
    aliases = {}
    if held is not None:
        in_specs.append(pl.BlockSpec(memory_space=pl.ANY))
        operands.append(held)
        aliases = {4: 0}
    return pl.pallas_call(
        step_kernel,
        grid=(steps,),
        in_specs=in_specs,
        out_specs=(
            block,
            pl.BlockSpec((groups, BLOCK // width, SUB, width), lambda i: (0, i, 0, 0)),
        ),
        out_shape=(
            jax.ShapeDtypeStruct((rows, cols), jnp.bfloat16),
            jax.ShapeDtypeStruct((groups, span // width, SUB, width), jnp.bfloat16),
        ),
        input_output_aliases=aliases,
        compiler_params=pltpu.CompilerParams(vmem_limit_bytes=24 << 20),
        name=f"local_step_{chunk}",
    )(*[pltpu.with_memory_space_constraint(a, pltpu.HBM) for a in operands])


def mixing_kernel(shift_ref, worker_ref, out_ref):
    workers = worker_ref.shape[1]
    half = workers // 2
    row = lax.broadcasted_iota(jnp.int32, (workers, workers), 0)
    col = lax.broadcasted_iota(jnp.int32, (workers, workers), 1)
    gap = (row - col) & (workers - 1)
    mix = (row == worker_ref[...]).astype(jnp.float32)
    for step in range(shift_ref.shape[0]):
        offset = jnp.left_shift(jnp.int32(1), shift_ref[step])
        one = ((gap == 0) | (gap == offset)).astype(jnp.bfloat16)
        mix = jnp.dot(one, mix.astype(jnp.bfloat16), preferred_element_type=jnp.float32)
    mix = mix[:half].astype(jnp.bfloat16)
    wide = workers * SUB
    spread_col = (
        lax.broadcasted_iota(jnp.int32, (workers, wide), 1) // SUB
        == lax.broadcasted_iota(jnp.int32, (workers, wide), 0)
    ).astype(jnp.bfloat16)
    wide_mix = jnp.dot(mix, spread_col, preferred_element_type=jnp.float32)
    out_ref[...] = wide_mix * (1.0 / workers)


def mixing(round_shift, held):
    workers = held.shape[1]
    return pl.pallas_call(
        mixing_kernel,
        in_specs=[
            pl.BlockSpec(memory_space=pltpu.SMEM),
            pl.BlockSpec(memory_space=pltpu.VMEM),
        ],
        out_specs=pl.BlockSpec(memory_space=pltpu.VMEM),
        out_shape=pltpu.VMEM((workers // 2, workers * SUB), jnp.float32),
        compiler_params=pltpu.CompilerParams(vmem_limit_bytes=24 << 20),
        name="mixing",
    )(round_shift, held)


def mix_kernel(mix_ref, rows_ref, out_ref, full_ref):
    half, wide = mix_ref.shape
    same = (
        lax.broadcasted_iota(jnp.int32, (SUB, wide), 1) & (SUB - 1)
        == lax.broadcasted_iota(jnp.int32, (SUB, wide), 0)
    )
    for at in range(0, half, 2):
        lines = [
            jnp.where(same, jnp.broadcast_to(mix_ref[k : k + 1], (SUB, wide)), 0.0)
            for k in (at, at + 1)
        ]
        full_ref[at * SUB : (at + 2) * SUB] = jnp.concatenate(lines, axis=0).astype(jnp.bfloat16)
    mixed = jnp.dot(full_ref[...], rows_ref[...], preferred_element_type=jnp.float32)
    mixed = mixed.astype(jnp.bfloat16)
    out_ref[: half * SUB] = mixed
    out_ref[half * SUB :] = mixed


def mix(matrix, rows):
    half, wide = matrix.shape
    return pl.pallas_call(
        mix_kernel,
        in_specs=[
            pl.BlockSpec(memory_space=pltpu.VMEM),
            pl.BlockSpec(memory_space=pltpu.VMEM),
        ],
        out_specs=pl.BlockSpec(memory_space=pltpu.VMEM),
        out_shape=pltpu.VMEM(rows.shape, jnp.bfloat16),
        scratch_shapes=[pltpu.VMEM((half * SUB, wide), jnp.bfloat16)],
        compiler_params=pltpu.CompilerParams(vmem_limit_bytes=24 << 20),
        name="mix",
    )(
        pltpu.with_memory_space_constraint(matrix, pltpu.VMEM),
        pltpu.with_memory_space_constraint(rows, pltpu.VMEM),
    )


def exchange(pieces):
    return lax.all_to_all(pieces, ("gx", "gy", "gz"), split_axis=0, concat_axis=0, tiled=True)


def shards(hidden_acts, output_grad, weights, momentum, worker_of_slot, round_shift):
    hidden = hidden_acts.reshape(hidden_acts.shape[-2:])
    grad_out = output_grad.reshape(output_grad.shape[-2:]).T
    weight = weights.reshape(weights.shape[-2:])
    moment = momentum.reshape(momentum.shape[-2:])
    count_x = lax.axis_size("gx")
    count_y = lax.axis_size("gy")
    count_z = lax.axis_size("gz")
    workers = count_x * count_y * count_z
    rows, cols = weight.shape
    groups = rows // SUB
    held = worker_of_slot.reshape(count_z, count_y, count_x).transpose(2, 1, 0)
    matrix = mixing(round_shift, held.reshape(1, workers))
    new_moment = None
    parts = []
    for chunk in range(CHUNKS):
        new_moment, pieces = local_step(chunk, grad_out, hidden, weight, moment, new_moment)
        parts.append(exchange(pieces.reshape(workers, SUB, -1)))
    mixed = []
    for part in parts:
        width = part.shape[-1]
        out = mix(matrix, part.reshape(workers * SUB, width))
        mixed.append(exchange(out.reshape(workers, SUB, width)))
    done = [
        part.reshape(groups, workers // groups, SUB, -1).transpose(0, 2, 1, 3).reshape(rows, -1)
        for part in mixed
    ]
    block = jnp.concatenate(done, axis=1) if CHUNKS > 1 else done[0]
    return (block.reshape(weights.shape), new_moment.reshape(momentum.shape))


def solution(mesh):
    placed = (
        P("gz", "gy", "gx", None, None),
        P("gz", "gy", "gx", None, None),
        P("gz", "gy", "gx", None, None),
        P("gz", "gy", "gx", None, None),
        P(),
        P(),
    )
    return jax.shard_map(
        shards,
        mesh=mesh,
        in_specs=placed,
        out_specs=(P("gx", "gy", "gz", None, None), P("gz", "gy", "gx", None, None)),
        check_vma=False,
    )
```

```python
import jax
import jax.numpy as jnp
from jax import lax
from jax.experimental import pallas as pl
from jax.experimental.pallas import tpu as pltpu
from jax.sharding import PartitionSpec as P


BLOCK = 8192
SUB = 8

learn_rate = 0.01
beta_keep = 0.9


def velocity_of(grad_out_ref, first_ref, second_ref, moment_ref):
    tokens = first_ref.shape[0]
    grad = jnp.dot(
        grad_out_ref[:, :tokens], first_ref[...], preferred_element_type=jnp.float32
    ) + jnp.dot(grad_out_ref[:, tokens:], second_ref[...], preferred_element_type=jnp.float32)
    return beta_keep * moment_ref[...].astype(jnp.float32) + grad


def step_kernel(grad_out_ref, first_ref, second_ref, weight_ref, moment_ref, pieces_ref):
    velocity = velocity_of(grad_out_ref, first_ref, second_ref, moment_ref)
    stepped = (weight_ref[...].astype(jnp.float32) - learn_rate * velocity).astype(jnp.bfloat16)
    groups, count, _, width = pieces_ref.shape
    for group in range(groups):
        for at in range(count):
            pieces_ref[group, at] = stepped[
                group * SUB : (group + 1) * SUB, at * width : (at + 1) * width
            ]


def moment_kernel(grad_out_ref, first_ref, second_ref, moment_ref, new_moment_ref):
    velocity = velocity_of(grad_out_ref, first_ref, second_ref, moment_ref)
    new_moment_ref[...] = velocity.astype(jnp.bfloat16)


def in_hbm(*operands):
    return [pltpu.with_memory_space_constraint(a, pltpu.HBM) for a in operands]


def local_step(grad_out, hidden, weight, moment, workers):
    rows, cols = weight.shape
    tokens = hidden.shape[0]
    groups = rows // SUB
    width = cols * groups // workers
    block = pl.BlockSpec((rows, BLOCK), lambda i: (0, i))
    return pl.pallas_call(
        step_kernel,
        grid=(cols // BLOCK,),
        in_specs=[
            pl.BlockSpec((rows, tokens), lambda i: (0, 0)),
            pl.BlockSpec((tokens // 2, BLOCK), lambda i: (0, i)),
            pl.BlockSpec((tokens // 2, BLOCK), lambda i: (1, i)),
            block,
            block,
        ],
        out_specs=pl.BlockSpec((groups, BLOCK // width, SUB, width), lambda i: (0, i, 0, 0)),
        out_shape=jax.ShapeDtypeStruct((groups, cols // width, SUB, width), jnp.bfloat16),
        compiler_params=pltpu.CompilerParams(vmem_limit_bytes=24 << 20),
        name="local_step",
    )(*in_hbm(grad_out, hidden, hidden, weight, moment))


def momentum_step(grad_out, hidden, moment):
    rows, cols = moment.shape
    tokens = hidden.shape[0]
    block = pl.BlockSpec((rows, BLOCK), lambda i: (0, i))
    return pl.pallas_call(
        moment_kernel,
        grid=(cols // BLOCK,),
        in_specs=[
            pl.BlockSpec((rows, tokens), lambda i: (0, 0)),
            pl.BlockSpec((tokens // 2, BLOCK), lambda i: (0, i)),
            pl.BlockSpec((tokens // 2, BLOCK), lambda i: (1, i)),
            block,
        ],
        out_specs=block,
        out_shape=jax.ShapeDtypeStruct((rows, cols), jnp.bfloat16),
        compiler_params=pltpu.CompilerParams(vmem_limit_bytes=24 << 20),
        name="momentum_step",
    )(*in_hbm(grad_out, hidden, hidden, moment))


def mixing_kernel(shift_ref, worker_ref, out_ref):
    workers = worker_ref.shape[1]
    half = workers // 2
    row = lax.broadcasted_iota(jnp.int32, (workers, workers), 0)
    col = lax.broadcasted_iota(jnp.int32, (workers, workers), 1)
    gap = (row - col) & (workers - 1)
    mix = (row == worker_ref[...]).astype(jnp.float32)
    for step in range(shift_ref.shape[0]):
        offset = jnp.left_shift(jnp.int32(1), shift_ref[step])
        one = ((gap == 0) | (gap == offset)).astype(jnp.bfloat16)
        mix = jnp.dot(one, mix.astype(jnp.bfloat16), preferred_element_type=jnp.float32)
    mix = mix[:half].astype(jnp.bfloat16)
    wide = workers * SUB
    spread_col = (
        lax.broadcasted_iota(jnp.int32, (workers, wide), 1) // SUB
        == lax.broadcasted_iota(jnp.int32, (workers, wide), 0)
    ).astype(jnp.bfloat16)
    wide_mix = jnp.dot(mix, spread_col, preferred_element_type=jnp.float32)
    out_ref[...] = wide_mix * (1.0 / workers)


def mixing(round_shift, held):
    workers = held.shape[1]
    return pl.pallas_call(
        mixing_kernel,
        in_specs=[
            pl.BlockSpec(memory_space=pltpu.SMEM),
            pl.BlockSpec(memory_space=pltpu.VMEM),
        ],
        out_specs=pl.BlockSpec(memory_space=pltpu.VMEM),
        out_shape=pltpu.VMEM((workers // 2, workers * SUB), jnp.float32),
        compiler_params=pltpu.CompilerParams(vmem_limit_bytes=24 << 20),
        name="mixing",
    )(round_shift, held)


def mix_kernel(mix_ref, rows_ref, out_ref, full_ref):
    half, wide = mix_ref.shape
    same = (
        lax.broadcasted_iota(jnp.int32, (SUB, wide), 1) & (SUB - 1)
        == lax.broadcasted_iota(jnp.int32, (SUB, wide), 0)
    )
    for at in range(0, half, 2):
        lines = [
            jnp.where(same, jnp.broadcast_to(mix_ref[k : k + 1], (SUB, wide)), 0.0)
            for k in (at, at + 1)
        ]
        full_ref[at * SUB : (at + 2) * SUB] = jnp.concatenate(lines, axis=0).astype(jnp.bfloat16)
    mixed = jnp.dot(full_ref[...], rows_ref[...], preferred_element_type=jnp.float32)
    mixed = mixed.astype(jnp.bfloat16)
    out_ref[: half * SUB] = mixed
    out_ref[half * SUB :] = mixed


def mix(matrix, rows):
    half, wide = matrix.shape
    return pl.pallas_call(
        mix_kernel,
        in_specs=[
            pl.BlockSpec(memory_space=pltpu.VMEM),
            pl.BlockSpec(memory_space=pltpu.VMEM),
        ],
        out_specs=pl.BlockSpec(memory_space=pltpu.VMEM),
        out_shape=pltpu.VMEM(rows.shape, jnp.bfloat16),
        scratch_shapes=[pltpu.VMEM((half * SUB, wide), jnp.bfloat16)],
        compiler_params=pltpu.CompilerParams(vmem_limit_bytes=24 << 20),
        name="mix",
    )(
        pltpu.with_memory_space_constraint(matrix, pltpu.VMEM),
        pltpu.with_memory_space_constraint(rows, pltpu.VMEM),
    )


def exchange(pieces):
    return lax.all_to_all(pieces, ("gx", "gy", "gz"), split_axis=0, concat_axis=0, tiled=True)


def shards(hidden_acts, output_grad, weights, momentum, worker_of_slot, round_shift):
    hidden = hidden_acts.reshape(hidden_acts.shape[-2:])
    grad_out = output_grad.reshape(output_grad.shape[-2:]).T
    weight = weights.reshape(weights.shape[-2:])
    moment = momentum.reshape(momentum.shape[-2:])
    count_x = lax.axis_size("gx")
    count_y = lax.axis_size("gy")
    count_z = lax.axis_size("gz")
    workers = count_x * count_y * count_z
    rows, _ = weight.shape
    groups = rows // SUB
    held = worker_of_slot.reshape(count_z, count_y, count_x).transpose(2, 1, 0)
    matrix = mixing(round_shift, held.reshape(1, workers))
    pieces = local_step(grad_out, hidden, weight, moment, workers)
    received = exchange(pieces.reshape(workers, SUB, -1))
    new_moment = momentum_step(grad_out, hidden, moment)
    width = received.shape[-1]
    mixed = mix(matrix, received.reshape(workers * SUB, width))
    returned = exchange(mixed.reshape(workers, SUB, width))
    block = returned.reshape(groups, workers // groups, SUB, width).transpose(0, 2, 1, 3)
    return (block.reshape(weights.shape), new_moment.reshape(momentum.shape))


def solution(mesh):
    placed = (
        P("gz", "gy", "gx", None, None),
        P("gz", "gy", "gx", None, None),
        P("gz", "gy", "gx", None, None),
        P("gz", "gy", "gx", None, None),
        P(),
        P(),
    )
    return jax.shard_map(
        shards,
        mesh=mesh,
        in_specs=placed,
        out_specs=(P("gx", "gy", "gz", None, None), P("gz", "gy", "gx", None, None)),
        check_vma=False,
    )
```

```python
import functools

import jax
import jax.numpy as jnp
from jax import lax
from jax.experimental import pallas as pl
from jax.experimental.pallas import tpu as pltpu
from jax.sharding import PartitionSpec as P


BLOCK = 8192
SUB = 8

learn_rate = 0.01
beta_keep = 0.9


def velocity_of(grad_out_ref, first_ref, second_ref, moment_ref):
    tokens = first_ref.shape[0]
    grad = jnp.dot(
        grad_out_ref[:, :tokens], first_ref[...], preferred_element_type=jnp.float32
    ) + jnp.dot(grad_out_ref[:, tokens:], second_ref[...], preferred_element_type=jnp.float32)
    return beta_keep * moment_ref[...].astype(jnp.float32) + grad


def step_kernel(grad_out_ref, first_ref, second_ref, weight_ref, moment_ref, pieces_ref):
    velocity = velocity_of(grad_out_ref, first_ref, second_ref, moment_ref)
    stepped = (weight_ref[...].astype(jnp.float32) - learn_rate * velocity).astype(jnp.bfloat16)
    groups, count, _, width = pieces_ref.shape
    for group in range(groups):
        for at in range(count):
            pieces_ref[group, at] = stepped[
                group * SUB : (group + 1) * SUB, at * width : (at + 1) * width
            ]


def moment_kernel(grad_out_ref, first_ref, second_ref, moment_ref, new_moment_ref):
    velocity = velocity_of(grad_out_ref, first_ref, second_ref, moment_ref)
    new_moment_ref[...] = velocity.astype(jnp.bfloat16)


def in_hbm(*operands):
    return [pltpu.with_memory_space_constraint(a, pltpu.HBM) for a in operands]


def local_step(grad_out, hidden, weight, moment, workers):
    rows, cols = weight.shape
    tokens = hidden.shape[0]
    groups = rows // SUB
    width = cols * groups // workers
    block = pl.BlockSpec((rows, BLOCK), lambda i: (0, i))
    return pl.pallas_call(
        step_kernel,
        grid=(cols // BLOCK,),
        in_specs=[
            pl.BlockSpec((rows, tokens), lambda i: (0, 0)),
            pl.BlockSpec((tokens // 2, BLOCK), lambda i: (0, i)),
            pl.BlockSpec((tokens // 2, BLOCK), lambda i: (1, i)),
            block,
            block,
        ],
        out_specs=pl.BlockSpec((groups, BLOCK // width, SUB, width), lambda i: (0, i, 0, 0)),
        out_shape=jax.ShapeDtypeStruct((groups, cols // width, SUB, width), jnp.bfloat16),
        compiler_params=pltpu.CompilerParams(vmem_limit_bytes=24 << 20),
        name="local_step",
    )(*in_hbm(grad_out, hidden, hidden, weight, moment))


def momentum_step(grad_out, hidden, moment):
    rows, cols = moment.shape
    tokens = hidden.shape[0]
    block = pl.BlockSpec((rows, BLOCK), lambda i: (0, i))
    return pl.pallas_call(
        moment_kernel,
        grid=(cols // BLOCK,),
        in_specs=[
            pl.BlockSpec((rows, tokens), lambda i: (0, 0)),
            pl.BlockSpec((tokens // 2, BLOCK), lambda i: (0, i)),
            pl.BlockSpec((tokens // 2, BLOCK), lambda i: (1, i)),
            block,
        ],
        out_specs=block,
        out_shape=jax.ShapeDtypeStruct((rows, cols), jnp.bfloat16),
        compiler_params=pltpu.CompilerParams(vmem_limit_bytes=24 << 20),
        name="momentum_step",
    )(*in_hbm(grad_out, hidden, hidden, moment))


def mixing_kernel(sizes, shift_ref, out_ref):
    _, count_y, count_z = sizes
    half = out_ref.shape[0]
    row = lax.broadcasted_iota(jnp.int32, (half, half), 0)
    col = lax.broadcasted_iota(jnp.int32, (half, half), 1)
    gap = (row - col) & (half - 1)
    place_x = row // (count_y * count_z)
    place_z = row // count_y % count_z
    place_y = row % count_y
    mix = ((place_x * count_y + place_y) * count_z + place_z == col).astype(jnp.float32)
    for step in range(shift_ref.shape[0]):
        offset = jnp.left_shift(jnp.int32(1), shift_ref[step]) & (half - 1)
        one = (gap == 0).astype(jnp.float32) + (gap == offset).astype(jnp.float32)
        mix = jnp.dot(
            mix.astype(jnp.bfloat16), one.astype(jnp.bfloat16), preferred_element_type=jnp.float32
        )
    wide = half * SUB
    spread_col = (
        lax.broadcasted_iota(jnp.int32, (half, wide), 1) // SUB
        == lax.broadcasted_iota(jnp.int32, (half, wide), 0)
    ).astype(jnp.bfloat16)
    wide_mix = jnp.dot(mix.astype(jnp.bfloat16), spread_col, preferred_element_type=jnp.float32)
    out_ref[...] = wide_mix * (0.5 / half)


def mixing(round_shift, sizes):
    half = sizes[0] * sizes[1] * sizes[2] // 2
    return pl.pallas_call(
        functools.partial(mixing_kernel, sizes),
        in_specs=[pl.BlockSpec(memory_space=pltpu.SMEM)],
        out_specs=pl.BlockSpec(memory_space=pltpu.VMEM),
        out_shape=pltpu.VMEM((half, half * SUB), jnp.float32),
        compiler_params=pltpu.CompilerParams(vmem_limit_bytes=24 << 20),
        name="mixing",
    )(round_shift)


def mix_kernel(place_ref, mix_ref, rows_ref, out_ref, full_ref, pair_ref):
    half, wide = mix_ref.shape
    same = (
        lax.broadcasted_iota(jnp.int32, (SUB, wide), 1) & (SUB - 1)
        == lax.broadcasted_iota(jnp.int32, (SUB, wide), 0)
    )
    for at in range(0, half, 2):
        pairs = [
            (
                rows_ref[place_ref[k]].astype(jnp.float32)
                + rows_ref[place_ref[k + half]].astype(jnp.float32)
            )
            * 0.5
            for k in (at, at + 1)
        ]
        pair_ref[at * SUB : (at + 2) * SUB] = jnp.concatenate(pairs, axis=0).astype(jnp.bfloat16)
        lines = [
            jnp.where(same, jnp.broadcast_to(mix_ref[k : k + 1], (SUB, wide)), 0.0)
            for k in (at, at + 1)
        ]
        full_ref[at * SUB : (at + 2) * SUB] = jnp.concatenate(lines, axis=0).astype(jnp.bfloat16)
    mixed = jnp.dot(full_ref[...], pair_ref[...], preferred_element_type=jnp.float32)
    mixed = mixed.astype(jnp.bfloat16)
    out_ref[:wide] = mixed
    out_ref[wide:] = mixed


def mix(places, matrix, rows):
    _, wide = matrix.shape
    width = rows.shape[-1]
    return pl.pallas_call(
        mix_kernel,
        in_specs=[
            pl.BlockSpec(memory_space=pltpu.SMEM),
            pl.BlockSpec(memory_space=pltpu.VMEM),
            pl.BlockSpec(memory_space=pltpu.VMEM),
        ],
        out_specs=pl.BlockSpec(memory_space=pltpu.VMEM),
        out_shape=pltpu.VMEM((2 * wide, width), jnp.bfloat16),
        scratch_shapes=[
            pltpu.VMEM((wide, wide), jnp.bfloat16),
            pltpu.VMEM((wide, width), jnp.bfloat16),
        ],
        compiler_params=pltpu.CompilerParams(vmem_limit_bytes=24 << 20),
        name="mix",
    )(
        places,
        pltpu.with_memory_space_constraint(matrix, pltpu.VMEM),
        pltpu.with_memory_space_constraint(rows, pltpu.VMEM),
    )


def exchange(pieces):
    return lax.all_to_all(pieces, ("gx", "gz", "gy"), split_axis=0, concat_axis=0, tiled=True)


def shards(hidden_acts, output_grad, weights, momentum, worker_of_slot, round_shift):
    hidden = hidden_acts.reshape(hidden_acts.shape[-2:])
    grad_out = output_grad.reshape(output_grad.shape[-2:]).T
    weight = weights.reshape(weights.shape[-2:])
    moment = momentum.reshape(momentum.shape[-2:])
    count_x = lax.axis_size("gx")
    count_y = lax.axis_size("gy")
    count_z = lax.axis_size("gz")
    workers = count_x * count_y * count_z
    rows, _ = weight.shape
    groups = rows // SUB
    held = worker_of_slot.reshape(count_z, count_y, count_x).transpose(2, 0, 1).reshape(1, workers)
    order = jnp.arange(workers, dtype=jnp.int32)
    places = jnp.sum(jnp.where(held == order[:, None], order[None, :], 0), axis=1, dtype=jnp.int32)
    matrix = mixing(round_shift, (count_x, count_y, count_z))
    pieces = local_step(grad_out, hidden, weight, moment, workers)
    received = exchange(pieces.reshape(workers, SUB, -1))
    new_moment = momentum_step(grad_out, hidden, moment)
    width = received.shape[-1]
    mixed = mix(places, matrix, received)
    returned = exchange(mixed.reshape(workers, SUB, width))
    block = returned.reshape(groups, workers // groups, SUB, width).transpose(0, 2, 1, 3)
    return (block.reshape(weights.shape), new_moment.reshape(momentum.shape))


def solution(mesh):
    placed = (
        P("gz", "gy", "gx", None, None),
        P("gz", "gy", "gx", None, None),
        P("gz", "gy", "gx", None, None),
        P("gz", "gy", "gx", None, None),
        P(),
        P(),
    )
    return jax.shard_map(
        shards,
        mesh=mesh,
        in_specs=placed,
        out_specs=(P("gx", "gy", "gz", None, None), P("gz", "gy", "gx", None, None)),
        check_vma=False,
    )
```

```python
import jax
import jax.numpy as jnp
from jax import lax
from jax.experimental import pallas as pl
from jax.experimental.pallas import tpu as pltpu
from jax.sharding import PartitionSpec as P


BLOCK = 8192
SUB = 8

learn_rate = 0.01
beta_keep = 0.9


def velocity_of(grad_out_ref, first_ref, second_ref, moment_ref):
    tokens = first_ref.shape[0]
    grad = jnp.dot(
        grad_out_ref[:, :tokens], first_ref[...], preferred_element_type=jnp.float32
    ) + jnp.dot(grad_out_ref[:, tokens:], second_ref[...], preferred_element_type=jnp.float32)
    return beta_keep * moment_ref[...].astype(jnp.float32) + grad


def step_kernel(grad_out_ref, first_ref, second_ref, weight_ref, moment_ref, pieces_ref):
    velocity = velocity_of(grad_out_ref, first_ref, second_ref, moment_ref)
    stepped = (weight_ref[...].astype(jnp.float32) - learn_rate * velocity).astype(jnp.bfloat16)
    groups, count, _, width = pieces_ref.shape
    for group in range(groups):
        for at in range(count):
            pieces_ref[group, at] = stepped[
                group * SUB : (group + 1) * SUB, at * width : (at + 1) * width
            ]


def moment_kernel(grad_out_ref, first_ref, second_ref, moment_ref, new_moment_ref):
    velocity = velocity_of(grad_out_ref, first_ref, second_ref, moment_ref)
    new_moment_ref[...] = velocity.astype(jnp.bfloat16)


def in_hbm(*operands):
    return [pltpu.with_memory_space_constraint(a, pltpu.HBM) for a in operands]


def local_step(grad_out, hidden, weight, moment, workers):
    rows, cols = weight.shape
    tokens = hidden.shape[0]
    groups = rows // SUB
    width = cols * groups // workers
    block = pl.BlockSpec((rows, BLOCK), lambda i: (0, i))
    return pl.pallas_call(
        step_kernel,
        grid=(cols // BLOCK,),
        in_specs=[
            pl.BlockSpec((rows, tokens), lambda i: (0, 0)),
            pl.BlockSpec((tokens // 2, BLOCK), lambda i: (0, i)),
            pl.BlockSpec((tokens // 2, BLOCK), lambda i: (1, i)),
            block,
            block,
        ],
        out_specs=pl.BlockSpec((groups, BLOCK // width, SUB, width), lambda i: (0, i, 0, 0)),
        out_shape=jax.ShapeDtypeStruct((groups, cols // width, SUB, width), jnp.bfloat16),
        compiler_params=pltpu.CompilerParams(vmem_limit_bytes=24 << 20),
        name="local_step",
    )(*in_hbm(grad_out, hidden, hidden, weight, moment))


def momentum_step(grad_out, hidden, moment):
    rows, cols = moment.shape
    tokens = hidden.shape[0]
    block = pl.BlockSpec((rows, BLOCK), lambda i: (0, i))
    return pl.pallas_call(
        moment_kernel,
        grid=(cols // BLOCK,),
        in_specs=[
            pl.BlockSpec((rows, tokens), lambda i: (0, 0)),
            pl.BlockSpec((tokens // 2, BLOCK), lambda i: (0, i)),
            pl.BlockSpec((tokens // 2, BLOCK), lambda i: (1, i)),
            block,
        ],
        out_specs=block,
        out_shape=jax.ShapeDtypeStruct((rows, cols), jnp.bfloat16),
        compiler_params=pltpu.CompilerParams(vmem_limit_bytes=24 << 20),
        name="momentum_step",
    )(*in_hbm(grad_out, hidden, hidden, moment))


def mixing_kernel(shift_ref, out_ref):
    wide = out_ref.shape[0]
    half = wide // SUB
    row = lax.broadcasted_iota(jnp.int32, (half, half), 0)
    col = lax.broadcasted_iota(jnp.int32, (half, half), 1)
    gap = (row - col) & (half - 1)
    mix = (gap == 0).astype(jnp.float32)
    for step in range(shift_ref.shape[0]):
        offset = jnp.left_shift(jnp.int32(1), shift_ref[step]) & (half - 1)
        one = (gap == 0).astype(jnp.float32) + (gap == offset).astype(jnp.float32)
        mix = jnp.dot(
            one.astype(jnp.bfloat16), mix.astype(jnp.bfloat16), preferred_element_type=jnp.float32
        )
    spread_col = (
        lax.broadcasted_iota(jnp.int32, (half, wide), 1) // SUB
        == lax.broadcasted_iota(jnp.int32, (half, wide), 0)
    ).astype(jnp.bfloat16)
    wide_mix = jnp.dot(mix.astype(jnp.bfloat16), spread_col, preferred_element_type=jnp.float32)
    wide_mix = wide_mix * (0.5 / half)
    same = (
        lax.broadcasted_iota(jnp.int32, (SUB, wide), 1) & (SUB - 1)
        == lax.broadcasted_iota(jnp.int32, (SUB, wide), 0)
    )
    for at in range(0, half, 2):
        lines = [
            jnp.where(same, jnp.broadcast_to(wide_mix[k : k + 1], (SUB, wide)), 0.0)
            for k in (at, at + 1)
        ]
        out_ref[at * SUB : (at + 2) * SUB] = jnp.concatenate(lines, axis=0).astype(jnp.bfloat16)


def mixing(round_shift, workers):
    wide = workers // 2 * SUB
    return pl.pallas_call(
        mixing_kernel,
        in_specs=[pl.BlockSpec(memory_space=pltpu.SMEM)],
        out_specs=pl.BlockSpec(memory_space=pltpu.VMEM),
        out_shape=pltpu.VMEM((wide, wide), jnp.bfloat16),
        compiler_params=pltpu.CompilerParams(vmem_limit_bytes=24 << 20),
        name="mixing",
    )(round_shift)


def mix_kernel(place_ref, mix_ref, rows_ref, out_ref, pair_ref):
    wide = mix_ref.shape[0]
    half = wide // SUB
    for at in range(0, half, 2):
        pairs = [
            (
                rows_ref[place_ref[k]].astype(jnp.float32)
                + rows_ref[place_ref[k + half]].astype(jnp.float32)
            )
            * 0.5
            for k in (at, at + 1)
        ]
        pair_ref[at * SUB : (at + 2) * SUB] = jnp.concatenate(pairs, axis=0).astype(jnp.bfloat16)
    mixed = jnp.dot(mix_ref[...], pair_ref[...], preferred_element_type=jnp.float32)
    mixed = mixed.astype(jnp.bfloat16)
    out_ref[:wide] = mixed
    out_ref[wide:] = mixed


def mix(places, matrix, rows):
    wide = matrix.shape[0]
    width = rows.shape[-1]
    return pl.pallas_call(
        mix_kernel,
        in_specs=[
            pl.BlockSpec(memory_space=pltpu.SMEM),
            pl.BlockSpec(memory_space=pltpu.VMEM),
            pl.BlockSpec(memory_space=pltpu.VMEM),
        ],
        out_specs=pl.BlockSpec(memory_space=pltpu.VMEM),
        out_shape=pltpu.VMEM((2 * wide, width), jnp.bfloat16),
        scratch_shapes=[pltpu.VMEM((wide, width), jnp.bfloat16)],
        compiler_params=pltpu.CompilerParams(vmem_limit_bytes=24 << 20),
        name="mix",
    )(
        places,
        pltpu.with_memory_space_constraint(matrix, pltpu.VMEM),
        pltpu.with_memory_space_constraint(rows, pltpu.VMEM),
    )


def exchange(pieces):
    return lax.all_to_all(pieces, ("gx", "gy", "gz"), split_axis=0, concat_axis=0, tiled=True)


def shards(hidden_acts, output_grad, weights, momentum, worker_of_slot, round_shift):
    hidden = hidden_acts.reshape(hidden_acts.shape[-2:])
    grad_out = output_grad.reshape(output_grad.shape[-2:]).T
    weight = weights.reshape(weights.shape[-2:])
    moment = momentum.reshape(momentum.shape[-2:])
    count_x = lax.axis_size("gx")
    count_y = lax.axis_size("gy")
    count_z = lax.axis_size("gz")
    workers = count_x * count_y * count_z
    rows, _ = weight.shape
    groups = rows // SUB
    held = worker_of_slot.reshape(count_z, count_y, count_x).transpose(2, 1, 0).reshape(1, workers)
    order = jnp.arange(workers, dtype=jnp.int32)
    places = jnp.sum(jnp.where(held == order[:, None], order[None, :], 0), axis=1, dtype=jnp.int32)
    matrix = mixing(round_shift, workers)
    pieces = local_step(grad_out, hidden, weight, moment, workers)
    received = exchange(pieces.reshape(workers, SUB, -1))
    new_moment = momentum_step(grad_out, hidden, moment)
    width = received.shape[-1]
    mixed = mix(places, matrix, received)
    returned = exchange(mixed.reshape(workers, SUB, width))
    block = returned.reshape(groups, workers // groups, SUB, width).transpose(0, 2, 1, 3)
    return (block.reshape(weights.shape), new_moment.reshape(momentum.shape))


def solution(mesh):
    placed = (
        P("gz", "gy", "gx", None, None),
        P("gz", "gy", "gx", None, None),
        P("gz", "gy", "gx", None, None),
        P("gz", "gy", "gx", None, None),
        P(),
        P(),
    )
    return jax.shard_map(
        shards,
        mesh=mesh,
        in_specs=placed,
        out_specs=(P("gx", "gy", "gz", None, None), P("gz", "gy", "gx", None, None)),
        check_vma=False,
    )
```

```python
import jax
import jax.numpy as jnp
from jax import lax
from jax.experimental import pallas as pl
from jax.experimental.pallas import tpu as pltpu
from jax.sharding import PartitionSpec as P


BLOCK = 8192
SUB = 8

learn_rate = 0.01
beta_keep = 0.9


def velocity_of(grad_out_ref, first_ref, second_ref, moment_ref):
    tokens = first_ref.shape[0]
    grad = jnp.dot(
        grad_out_ref[:, :tokens], first_ref[...], preferred_element_type=jnp.float32
    ) + jnp.dot(grad_out_ref[:, tokens:], second_ref[...], preferred_element_type=jnp.float32)
    return beta_keep * moment_ref[...].astype(jnp.float32) + grad


def step_kernel(grad_out_ref, first_ref, second_ref, weight_ref, moment_ref, pieces_ref):
    velocity = velocity_of(grad_out_ref, first_ref, second_ref, moment_ref)
    stepped = (weight_ref[...].astype(jnp.float32) - learn_rate * velocity).astype(jnp.bfloat16)
    groups, count, _, width = pieces_ref.shape
    for group in range(groups):
        for at in range(count):
            pieces_ref[group, at] = stepped[
                group * SUB : (group + 1) * SUB, at * width : (at + 1) * width
            ]


def moment_kernel(grad_out_ref, first_ref, second_ref, moment_ref, new_moment_ref):
    velocity = velocity_of(grad_out_ref, first_ref, second_ref, moment_ref)
    new_moment_ref[...] = velocity.astype(jnp.bfloat16)


def in_hbm(*operands):
    return [pltpu.with_memory_space_constraint(a, pltpu.HBM) for a in operands]


def local_step(grad_out, hidden, weight, moment, workers):
    rows, cols = weight.shape
    tokens = hidden.shape[0]
    groups = rows // SUB
    width = cols * groups // workers
    block = pl.BlockSpec((rows, BLOCK), lambda i: (0, i))
    return pl.pallas_call(
        step_kernel,
        grid=(cols // BLOCK,),
        in_specs=[
            pl.BlockSpec((rows, tokens), lambda i: (0, 0)),
            pl.BlockSpec((tokens // 2, BLOCK), lambda i: (0, i)),
            pl.BlockSpec((tokens // 2, BLOCK), lambda i: (1, i)),
            block,
            block,
        ],
        out_specs=pl.BlockSpec((groups, BLOCK // width, SUB, width), lambda i: (0, i, 0, 0)),
        out_shape=jax.ShapeDtypeStruct((groups, cols // width, SUB, width), jnp.bfloat16),
        compiler_params=pltpu.CompilerParams(vmem_limit_bytes=24 << 20),
        name="local_step",
    )(*in_hbm(grad_out, hidden, hidden, weight, moment))


def momentum_step(grad_out, hidden, moment):
    rows, cols = moment.shape
    tokens = hidden.shape[0]
    block = pl.BlockSpec((rows, BLOCK), lambda i: (0, i))
    return pl.pallas_call(
        moment_kernel,
        grid=(cols // BLOCK,),
        in_specs=[
            pl.BlockSpec((rows, tokens), lambda i: (0, 0)),
            pl.BlockSpec((tokens // 2, BLOCK), lambda i: (0, i)),
            pl.BlockSpec((tokens // 2, BLOCK), lambda i: (1, i)),
            block,
        ],
        out_specs=block,
        out_shape=jax.ShapeDtypeStruct((rows, cols), jnp.bfloat16),
        compiler_params=pltpu.CompilerParams(vmem_limit_bytes=24 << 20),
        name="momentum_step",
    )(*in_hbm(grad_out, hidden, hidden, moment))


def mixing_kernel(shift_ref, out_ref):
    wide = out_ref.shape[0]
    half = wide // SUB
    row = lax.broadcasted_iota(jnp.int32, (half, half), 0)
    col = lax.broadcasted_iota(jnp.int32, (half, half), 1)
    gap = (row - col) & (half - 1)
    mix = (gap == 0).astype(jnp.float32)
    for step in range(shift_ref.shape[0]):
        offset = jnp.left_shift(jnp.int32(1), shift_ref[step]) & (half - 1)
        one = (gap == 0).astype(jnp.float32) + (gap == offset).astype(jnp.float32)
        mix = jnp.dot(
            one.astype(jnp.bfloat16), mix.astype(jnp.bfloat16), preferred_element_type=jnp.float32
        )
    spread_col = (
        lax.broadcasted_iota(jnp.int32, (half, wide), 1) // SUB
        == lax.broadcasted_iota(jnp.int32, (half, wide), 0)
    ).astype(jnp.bfloat16)
    wide_mix = jnp.dot(mix.astype(jnp.bfloat16), spread_col, preferred_element_type=jnp.float32)
    wide_mix = wide_mix * (0.25 / half)
    same = (
        lax.broadcasted_iota(jnp.int32, (SUB, wide), 1) & (SUB - 1)
        == lax.broadcasted_iota(jnp.int32, (SUB, wide), 0)
    )
    for at in range(0, half, 2):
        lines = [
            jnp.where(same, jnp.broadcast_to(wide_mix[k : k + 1], (SUB, wide)), 0.0)
            for k in (at, at + 1)
        ]
        out_ref[at * SUB : (at + 2) * SUB] = jnp.concatenate(lines, axis=0).astype(jnp.bfloat16)


def mixing(round_shift, workers):
    wide = workers // 2 * SUB
    return pl.pallas_call(
        mixing_kernel,
        in_specs=[pl.BlockSpec(memory_space=pltpu.SMEM)],
        out_specs=pl.BlockSpec(memory_space=pltpu.VMEM),
        out_shape=pltpu.VMEM((wide, wide), jnp.bfloat16),
        compiler_params=pltpu.CompilerParams(vmem_limit_bytes=24 << 20),
        name="mixing",
    )(round_shift)


def mix_kernel(place_ref, mix_ref, rows_ref, out_ref, pair_ref):
    wide = mix_ref.shape[0]
    half = wide // SUB
    for at in range(0, half, 2):
        pairs = [rows_ref[place_ref[k]] + rows_ref[place_ref[k + half]] for k in (at, at + 1)]
        pair_ref[at * SUB : (at + 2) * SUB] = jnp.concatenate(pairs, axis=0)
    mixed = jnp.dot(mix_ref[...], pair_ref[...], preferred_element_type=jnp.float32)
    mixed = mixed.astype(jnp.bfloat16)
    out_ref[:wide] = mixed
    out_ref[wide:] = mixed


def mix(places, matrix, rows):
    wide = matrix.shape[0]
    width = rows.shape[-1]
    return pl.pallas_call(
        mix_kernel,
        in_specs=[
            pl.BlockSpec(memory_space=pltpu.SMEM),
            pl.BlockSpec(memory_space=pltpu.VMEM),
            pl.BlockSpec(memory_space=pltpu.VMEM),
        ],
        out_specs=pl.BlockSpec(memory_space=pltpu.VMEM),
        out_shape=pltpu.VMEM((2 * wide, width), jnp.bfloat16),
        scratch_shapes=[pltpu.VMEM((wide, width), jnp.bfloat16)],
        compiler_params=pltpu.CompilerParams(vmem_limit_bytes=24 << 20),
        name="mix",
    )(
        places,
        pltpu.with_memory_space_constraint(matrix, pltpu.VMEM),
        pltpu.with_memory_space_constraint(rows, pltpu.VMEM),
    )


def exchange(pieces):
    return lax.all_to_all(pieces, ("gx", "gy", "gz"), split_axis=0, concat_axis=0, tiled=True)


def shards(hidden_acts, output_grad, weights, momentum, worker_of_slot, round_shift):
    hidden = hidden_acts.reshape(hidden_acts.shape[-2:])
    grad_out = output_grad.reshape(output_grad.shape[-2:]).T
    weight = weights.reshape(weights.shape[-2:])
    moment = momentum.reshape(momentum.shape[-2:])
    count_x = lax.axis_size("gx")
    count_y = lax.axis_size("gy")
    count_z = lax.axis_size("gz")
    workers = count_x * count_y * count_z
    rows, _ = weight.shape
    groups = rows // SUB
    held = worker_of_slot.reshape(count_z, count_y, count_x).transpose(2, 1, 0).reshape(1, workers)
    order = jnp.arange(workers, dtype=jnp.int32)
    places = jnp.sum(jnp.where(held == order[:, None], order[None, :], 0), axis=1, dtype=jnp.int32)
    matrix = mixing(round_shift, workers)
    pieces = local_step(grad_out, hidden, weight, moment, workers)
    received = exchange(pieces.reshape(workers, SUB, -1))
    new_moment = momentum_step(grad_out, hidden, moment)
    width = received.shape[-1]
    mixed = mix(places, matrix, received)
    returned = exchange(mixed.reshape(workers, SUB, width))
    block = returned.reshape(groups, workers // groups, SUB, width).transpose(0, 2, 1, 3)
    return (block.reshape(weights.shape), new_moment.reshape(momentum.shape))


def solution(mesh):
    placed = (
        P("gz", "gy", "gx", None, None),
        P("gz", "gy", "gx", None, None),
        P("gz", "gy", "gx", None, None),
        P("gz", "gy", "gx", None, None),
        P(),
        P(),
    )
    return jax.shard_map(
        shards,
        mesh=mesh,
        in_specs=placed,
        out_specs=(P("gx", "gy", "gz", None, None), P("gz", "gy", "gx", None, None)),
        check_vma=False,
    )
```
